32 devices in a mesh: groups: 2 (over x), gx: 8 (over z, y), shot: 2 (over core).
Axes of the slice: x: 2, y: 2, z: 4, core: 2. Of those that a mesh axis runs over, the one named last changes fastest.
Arguments:
- src_now: float32 [8, 128, 64, 128], P(('groups', 'shot'), 'gx'), parts along dimension 0, may hold values from -6 to 6
- src_prev: float32 [8, 128, 64, 128], P(('groups', 'shot'), 'gx'), parts along dimension 0, may hold values from -6 to 6
- rec_now: float32 [8, 128, 64, 128], P(('groups', 'shot'), 'gx'), parts along dimension 0, may hold values from -6 to 6
- rec_prev: float32 [8, 128, 64, 128], P(('groups', 'shot'), 'gx'), parts along dimension 0, may hold values from -6 to 6
- courant_sq: float32 [256, 64, 128], P(('groups', 'gx')), parts along dimension 0, may hold values from 0.05 to 0.3
- wavelet: float32 [8, 4], P(('groups', 'shot')), parts along dimension 0, may hold values from -8 to 8
- traces: float32 [8, 4, 128], P(('groups', 'shot'), None, 'gx'), parts along dimension 0, may hold values from -6 to 6
- positions: int32 [8, 4], P(('groups', 'shot')), parts along dimension 0, may hold values from 0 to 127, as said below
Outputs:
- angle_image: float32 [16, 128, 32, 128], P(('groups', 'shot'), 'gx'), parts along dimension 0
The draws below stay inside these ranges and needn't reach their ends.
There are 2 independent parts, one for each index of `groups`. The reference program is written for one: setup_inputs(seed, part) draws one part's arguments, and reference() takes and returns one part's arrays. A program takes and returns all parts, laid end to end along the dimension named above; each array names one. Nothing has to cross between parts.
Inputs may be any that keep to these rules, and one draw needn't show every extreme that they name: `positions`: column 0 lies in 0 .. 127, columns 1 and 3 in 0 .. 127, column 2 in 0 .. 63; one shot of each patch has its source at x 128 - 1, y * 128 - 1, depth 64 - 1 and its receiver line at y 0.
All inputs are finite; a program needn't handle non-finite values.
Results may differ from the reference program's by a relative error of at most 0.0001.
Values sent between devices are 32-bit elements; how exact they have to be, the bound alone decides.
No kernel may reach another device: no remote copies, remote signals or barrier semaphores. Data moves between devices by JAX's collectives and lax.ppermute only.
A program may use at most 192 MiB of HBM per device.

```python
import math
import jax
import jax.numpy as jnp
from jax import lax

NY = 128
NZ = 64
STEPS = 4
IMAGES = 2
LAGS = 49
ANGLES = 8
HALF = 24
NZH = 32
NX = 128
SHOTS = 4


def draw_positions(key, part):
    limits = jnp.array([NX, NY, NZ, NY], jnp.int32)
    raw = jax.random.randint(jax.random.fold_in(key, 7), (SHOTS, 4), 0, 1 << 20, dtype=jnp.int32)
    drawn = raw % limits[None, :]
    corner = jnp.array([NX - 1, NY - 1, NZ - 1, 0], jnp.int32)
    return drawn.at[0].set(corner)


def block_scale(rng, dims, cuts, least, top_value):
    gain = 1.0
    for axis_at, blocks in cuts:
        steps = jax.random.uniform(jax.random.fold_in(jax.random.fold_in(rng, 6), axis_at), (blocks,), jnp.float32, least / len(cuts), top_value / len(cuts))
        gain = gain * jnp.repeat(jnp.exp(steps), dims[axis_at] // blocks).reshape((-1,) + (1,) * (len(dims) - 1 - axis_at))
    return gain


def gaussian(key, shape, scale, reach, pieces=(), kind=jnp.bfloat16):
    entries = scale * jax.random.normal(key, shape, jnp.float32)
    if pieces:
        entries = entries * block_scale(key, shape, pieces, -0.22, 0.18)
    return jnp.clip(entries, -reach, reach).astype(kind)


def setup_inputs(seed: int = 0, part: int = 0) -> dict:
    seeds = jax.random.split(jax.random.key(seed), 9)
    part_keys = jax.random.split(jax.random.fold_in(seeds[8], part), 9)
    return {
        "src_now": gaussian(part_keys[0], (SHOTS, NX, NZ, NY), 1.0, 6.0, ((0, 2), (1, 8)), jnp.float32),
        "src_prev": gaussian(part_keys[1], (SHOTS, NX, NZ, NY), 1.0, 6.0, ((0, 2), (1, 8)), jnp.float32),
        "rec_now": gaussian(part_keys[2], (SHOTS, NX, NZ, NY), 1.0, 6.0, ((0, 2), (1, 8)), jnp.float32),
        "rec_prev": gaussian(part_keys[3], (SHOTS, NX, NZ, NY), 1.0, 6.0, ((0, 2), (1, 8)), jnp.float32),
        "courant_sq": jnp.clip(jnp.exp(math.log(0.3) - 1.7917595 * jax.random.uniform(part_keys[4], (NX, NZ, NY), jnp.float32) ** block_scale(part_keys[4], (NX, NZ, NY), ((0, 8),), -0.2, 0.2)), 0.05, 0.3),
        "wavelet": gaussian(part_keys[5], (SHOTS, STEPS), 2.0, 8.0, ((0, 2),), jnp.float32),
        "traces": gaussian(part_keys[6], (SHOTS, STEPS, NX), 1.0, 6.0, ((0, 2), (2, 8)), jnp.float32),
        "positions": draw_positions(jax.random.fold_in(jax.random.fold_in(seeds[8], part), 71), part),
    }


def laplace(field):
    padded = jnp.pad(field, ((0, 0), (1, 1), (1, 1), (1, 1)))
    beside = padded[:, 2:, 1:-1, 1:-1] + padded[:, :-2, 1:-1, 1:-1]
    beside = beside + padded[:, 1:-1, 2:, 1:-1] + padded[:, 1:-1, :-2, 1:-1]
    beside = beside + padded[:, 1:-1, 1:-1, 2:] + padded[:, 1:-1, 1:-1, :-2]
    return beside - 6.0 * field

def slant_stack(source, receiver):
    width = source.shape[1]
    spad = jnp.pad(source, ((0, 0), (HALF, HALF), (0, 0), (0, 0)))
    rpad = jnp.pad(receiver, ((0, 0), (HALF, HALF), (0, 0), (0, 0)))
    totals = [None] * ANGLES
    for index in range(LAGS):
        offset = index - HALF
        product = lax.optimization_barrier(jnp.sum(spad[:, HALF - offset:HALF - offset + width] * rpad[:, HALF + offset:HALF + offset + width], axis=0))
        for angle in range(ANGLES):
            moved = angle * abs(offset) // ANGLES
            piece = product[:, moved:moved + NZH, :]
            totals[angle] = piece if totals[angle] is None else totals[angle] + piece
    return jnp.stack(totals)

def reference(src_now, src_prev, rec_now, rec_prev, courant_sq, wavelet, traces, positions):
    ftype = src_now.dtype
    xgrid = jnp.arange(NX, dtype=jnp.int32)
    ygrid = jnp.arange(NY, dtype=jnp.int32)
    zgrid = jnp.arange(NZ, dtype=jnp.int32)
    source_mask = ((xgrid[None, :, None, None] == positions[:, 0, None, None, None]) & (zgrid[None, None, :, None] == positions[:, 2, None, None, None]) & (ygrid[None, None, None, :] == positions[:, 1, None, None, None])).astype(ftype)
    line_mask = (ygrid[None, :] == positions[:, 3, None]).astype(ftype)
    every = STEPS // IMAGES
    total = jnp.zeros((ANGLES, NX, NZH, NY), ftype)
    for step in range(STEPS):
        src_next = 2.0 * src_now - src_prev + courant_sq[None] * laplace(src_now) + wavelet[:, step, None, None, None] * source_mask
        rec_next = 2.0 * rec_now - rec_prev + courant_sq[None] * laplace(rec_now)
        rec_next = rec_next.at[:, :, 0, :].add(traces[:, STEPS - 1 - step, :, None] * line_mask[:, None, :])
        src_prev, src_now = (src_now, src_next)
        rec_prev, rec_now = (rec_now, rec_next)
        if (step + 1) % every == 0:
            total = total + slant_stack(src_now, rec_now)
    return total * (1.0 / math.sqrt(LAGS * SHOTS * IMAGES))
```

```python
import functools
import math

import jax
import jax.numpy as jnp
from jax import lax
from jax.experimental import pallas as pl
from jax.experimental.pallas import tpu as pltpu
from jax.sharding import PartitionSpec as P

STEPS = 4
IMAGES = 2
LAGS = 49
ANGLES = 8
HALF = (LAGS - 1) // 2

VMEM = pl.BlockSpec(memory_space=pltpu.VMEM)
SMEM = pl.BlockSpec(memory_space=pltpu.SMEM)


def rows_needed(depth_out):
    deepest = depth_out + (ANGLES - 1) * HALF // ANGLES
    return -(-deepest // 8) * 8


def step_kernel(
    step, packing, where_ref, pos_ref, wav_ref, tr_ref,
    src_ref, rec_ref, srcp_ref, recp_ref, csq_ref, low_ref, high_ref, *outs
):
    srcn_ref, recn_ref, lo_ref, hi_ref = outs[:4]
    shots, planes, depth, ny = src_ref.shape
    now = [(src_ref, s) for s in range(shots)] + [(rec_ref, s) for s in range(shots)]
    prev = [(srcp_ref, s) for s in range(shots)] + [(recp_ref, s) for s in range(shots)]
    nxt = [(srcn_ref, s) for s in range(shots)] + [(recn_ref, s) for s in range(shots)]
    row = lax.broadcasted_iota(jnp.int32, (depth, ny), 0)
    lane = lax.broadcasted_iota(jnp.int32, (depth, ny), 1)
    lane1 = lax.broadcasted_iota(jnp.int32, (1, ny), 1)

    def plane(x, below, above):
        csq = csq_ref[x]
        for f in range(2 * shots):
            ref, s = now[f]
            c = ref[s, x]
            beside = below(f) + above(f)
            beside = beside + jnp.where(row == 0, 0.0, pltpu.roll(c, 1, 0))
            beside = beside + jnp.where(row == depth - 1, 0.0, pltpu.roll(c, depth - 1, 0))
            beside = beside + jnp.where(lane == 0, 0.0, pltpu.roll(c, 1, 1))
            beside = beside + jnp.where(lane == ny - 1, 0.0, pltpu.roll(c, ny - 1, 1))
            pref, _ = prev[f]
            out, _ = nxt[f]
            out[s, x] = 2.0 * c - pref[s, x] + csq * (beside - 6.0 * c)
            if f >= shots:
                add = jnp.where(lane1 == pos_ref[s, 3], tr_ref[s, STEPS - 1 - step, x], 0.0)
                out[s, x, 0:1, :] = out[s, x, 0:1, :] + add

    def inner(f, x):
        ref, s = now[f]
        return ref[s, x]

    plane(0, lambda f: low_ref[f], lambda f: inner(f, 1))
    plane(planes - 1, lambda f: inner(f, planes - 2), lambda f: high_ref[f])

    @pl.loop(1, planes - 1)
    def _(x):
        plane(x, lambda f: inner(f, x - 1), lambda f: inner(f, x + 1))

    for s in range(shots):
        at = pos_ref[s, 0] - where_ref[0] * planes

        @pl.when((at >= 0) & (at < planes))
        def _():
            z = pos_ref[s, 2]
            add = jnp.where(lane1 == pos_ref[s, 1], wav_ref[s, step], 0.0)
            srcn_ref[s, at, pl.ds(z, 1), :] = srcn_ref[s, at, pl.ds(z, 1), :] + add

    for f in range(2 * shots):
        out, s = nxt[f]
        lo_ref[f] = out[s, 0]
        hi_ref[f] = out[s, planes - 1]
    if packing:
        keep_ref, send_ref = outs[4:]
        rows = keep_ref.shape[2]
        width = ny // shots
        left = lax.broadcasted_iota(jnp.int32, (rows, ny), 1) < width
        first = where_ref[1] == 0

        @pl.loop(0, planes)
        def _(x):
            for field, ref in enumerate((srcn_ref, recn_ref)):
                a = ref[0, x, :rows]
                b = ref[1, x, :rows]
                lows = jnp.where(left, a, pltpu.roll(b, width, 1))
                highs = jnp.where(left, pltpu.roll(a, width, 1), b)
                keep_ref[field, x] = jnp.where(first, lows, highs)
                send_ref[field, x] = jnp.where(first, highs, lows)


def image_kernel(
    last, where_ref, keep_ref, swap_ref, below1_ref, below2_ref, above1_ref, above2_ref, *rest
):
    outs = rest[-8:-4]
    olds = rest[:4] if last else None
    win_ref, j_ref, d_ref, a_ref = rest[-4:]
    planes = keep_ref.shape[1]
    chunk = planes // 2
    depth_out = outs[0].shape[2]
    rows = keep_ref.shape[2]
    ny = keep_ref.shape[3]
    width = ny // 2
    y = where_ref[1]
    core = where_ref[2]
    far = jnp.where(y == 0, 0, 1)

    def place(piece, count, at):
        @pl.loop(0, count)
        def _(i):
            for field in range(2):
                win_ref[field, at + i] = piece[field, i]

    place(keep_ref, planes, HALF + far * planes)
    place(swap_ref, planes, HALF + (1 - far) * planes)
    place(below1_ref, chunk, far * 2 * chunk)
    place(below2_ref, planes, (1 - far) * chunk)
    place(above1_ref, chunk, HALF + 2 * planes + far * 2 * chunk)
    place(above2_ref, planes, HALF + 2 * planes + (1 - far) * chunk)

    left = lax.broadcasted_iota(jnp.int32, (depth_out, ny), 1) < width

    def product(x, h):
        u, v = HALF + x - h, HALF + x + h
        if h == 0:
            return win_ref[0, u] * win_ref[1, u]
        return win_ref[0, u] * win_ref[1, v] + win_ref[0, v] * win_ref[1, u]

    def slants(x, bank):
        totals = [None] * ANGLES

        def add(angle, slot, moved):
            piece = d_ref[bank, slot, moved : moved + depth_out, :]
            totals[angle] = piece if totals[angle] is None else totals[angle] + piece

        slot = 0
        for h in range(0, HALF + 1, 2):
            one = product(x, h)
            moves = [angle * h // ANGLES for angle in range(ANGLES)]
            if h + 1 > HALF:
                d_ref[bank, slot, :rows] = one
                for angle in range(ANGLES):
                    add(angle, slot, moves[angle])
                slot += 1
                continue
            two = product(x, h + 1)
            gaps = [angle * (h + 1) // ANGLES - moves[angle] for angle in range(ANGLES)]
            for gap in sorted(set(gaps)):
                if gap == 0:
                    both = one + two
                else:
                    j_ref[bank, h // 2, :rows] = two
                    both = one + j_ref[bank, h // 2, gap : gap + rows]
                d_ref[bank, slot, :rows] = both
                for angle in range(ANGLES):
                    if gaps[angle] == gap:
                        add(angle, slot, moves[angle])
                slot += 1
        return totals

    def fold(v):
        return v + pltpu.roll(v, width, 1)

    for part in range(2):
        slab = y if part == 0 else 1 - y
        mine_ref, theirs_ref = outs[part], outs[2 + part]

        @pl.loop(0, chunk)
        def _(i):
            x = slab * planes + i
            for angle, v in enumerate(slants(x, 0)):
                a_ref[angle] = fold(v)
            packed = []
            for angle, v in enumerate(slants(x + chunk, 1)):
                packed.append(jnp.where(left, a_ref[angle], fold(v)))
            group = ANGLES // 2
            for j in range(group):
                mine = jnp.where(core == 0, packed[j], packed[group + j])
                theirs = jnp.where(core == 0, packed[group + j], packed[j])
                if last:
                    mine = mine + olds[part][j, i]
                    theirs = theirs + olds[2 + part][j, i]
                mine_ref[j, i] = mine
                theirs_ref[j, i] = theirs


def final_kernel(scale, where_ref, keep_ref, other_ref, swap_ref, out_ref):
    angles, chunk, depth_out, ny = keep_ref.shape
    width = ny // 2
    left = lax.broadcasted_iota(jnp.int32, (depth_out, ny), 1) < width
    first = where_ref[1] == 0

    @pl.loop(0, chunk)
    def _(i):
        for a in range(angles):
            own = (keep_ref[a, i] + other_ref[a, i]) * scale
            got = swap_ref[a, i] * scale
            lows = jnp.where(first, own, got)
            highs = jnp.where(first, got, own)
            out_ref[a, i] = jnp.where(left, lows, pltpu.roll(highs, width, 1))
            out_ref[a, chunk + i] = jnp.where(left, pltpu.roll(lows, width, 1), highs)


def call(kernel, out_shape, n_smem, n_vmem, scratch=(), flops=1_000_000, name=None):
    return pl.pallas_call(
        kernel,
        out_shape=out_shape,
        in_specs=[SMEM] * n_smem + [VMEM] * n_vmem,
        out_specs=jax.tree.map(lambda _: VMEM, out_shape),
        scratch_shapes=list(scratch),
        cost_estimate=pl.CostEstimate(flops=flops, bytes_accessed=1_000_000, transcendentals=0),
        name=name,
    )


def local(src_now, src_prev, rec_now, rec_prev, courant_sq, wavelet, traces, positions):
    shots, planes, depth, ny = src_now.shape
    depth_out = depth // 2
    rows = min(depth, rows_needed(depth_out))
    chunk = planes // 2
    assert shots == 2 and HALF == 3 * chunk and planes == 2 * chunk
    count = lax.axis_size("gx")
    assert count % 2 == 0
    here = lax.axis_index("gx")
    where = jnp.stack([here, here % 2, lax.axis_index("shot")]).astype(jnp.int32)
    even = here % 2 == 0
    f32 = jnp.float32
    shape = jax.ShapeDtypeStruct

    def hop(value, steps):
        pairs = [(i, i + steps) for i in range(count) if 0 <= i + steps < count]
        return lax.ppermute(value, "gx", pairs)

    def swap(value):
        return lax.ppermute(value, "gx", [(i, i ^ 1) for i in range(count)])

    edge = shape((2 * shots, depth, ny), f32)
    field = shape(src_now.shape, f32)
    piece = shape((2, planes, rows, ny), f32)
    half_image = shape((ANGLES // 2, chunk, depth_out, ny), f32)

    lo = jnp.concatenate([src_now[:, 0], rec_now[:, 0]])
    hi = jnp.concatenate([src_now[:, -1], rec_now[:, -1]])
    every = STEPS // IMAGES
    total = None
    src, rec = src_now, rec_now
    for step in range(STEPS):
        low = hop(hi, 1)
        high = hop(lo, -1)
        packing = (step + 1) % every == 0
        out_shape = [field, field, edge, edge] + ([piece, piece] if packing else [])
        got = call(
            functools.partial(step_kernel, step, packing), out_shape, 4, 7, name=f"step{step}"
        )(where, positions, wavelet, traces, src, rec, src_prev, rec_prev, courant_sq, low, high)
        src_prev, rec_prev = src, rec
        src, rec, lo, hi = got[:4]
        if packing:
            keep, send = got[4:]
            up1 = hop(keep[:, chunk:], 2)
            down1 = hop(keep[:, :chunk], -2)
            other = swap(send)
            up2 = jnp.where(
                even, other, jnp.concatenate([other[:, chunk:], keep[:, :chunk]], axis=1)
            )
            down2 = jnp.where(
                even, jnp.concatenate([keep[:, chunk:], other[:, :chunk]], axis=1), other
            )
            up2 = hop(up2, 2)
            down2 = hop(down2, -2)
            last = total is not None
            scratch = [
                pltpu.VMEM((2, 2 * planes + 2 * HALF, rows, ny), f32),
                pltpu.VMEM((2, HALF // 2 + 1, rows + 8, ny), f32),
                pltpu.VMEM((2, HALF + 1, rows, ny), f32),
                pltpu.VMEM((ANGLES, depth_out, ny), f32),
            ]
            total = call(
                functools.partial(image_kernel, last), [half_image] * 4, 1, 10 if last else 6,
                scratch, flops=60_000_000, name=f"image{step}",
            )(where, keep, other, up1, up2, down1, down2, *(total if last else ()))
    mine_keep, mine_send, theirs_keep, theirs_send = total
    both = [(0, 1), (1, 0)]
    got_send = lax.ppermute(theirs_send, "shot", both)
    got_keep = lax.ppermute(theirs_keep, "shot", both)
    swapped = swap(mine_send + got_send)
    shots_all = shots * lax.axis_size("shot")
    scale = 1.0 / math.sqrt(LAGS * shots_all * IMAGES)
    return call(
        functools.partial(final_kernel, scale),
        shape((ANGLES // 2, planes, depth_out, ny), f32), 1, 3, name="final",
    )(where, mine_keep, got_keep, swapped)


def solution(mesh):
    placed = (
        P(("groups", "shot"), "gx", None, None),
        P(("groups", "shot"), "gx", None, None),
        P(("groups", "shot"), "gx", None, None),
        P(("groups", "shot"), "gx", None, None),
        P(("groups", "gx"), None, None),
        P(("groups", "shot"), None),
        P(("groups", "shot"), None, "gx"),
        P(("groups", "shot"), None),
    )
    return jax.shard_map(
        local,
        mesh=mesh,
        in_specs=placed,
        out_specs=P(("groups", "shot"), "gx", None, None),
        check_vma=False,
    )
```

```python
import functools
import math

import jax
import jax.numpy as jnp
from jax import lax
from jax.experimental import pallas as pl
from jax.experimental.pallas import tpu as pltpu
from jax.sharding import PartitionSpec as P


STEPS = 4
IMAGES = 2
LAGS = 49
ANGLES = 8
HALF = (LAGS - 1) // 2

VMEM = pl.BlockSpec(memory_space=pltpu.VMEM)
SMEM = pl.BlockSpec(memory_space=pltpu.SMEM)
HBM = pl.BlockSpec(memory_space=pltpu.HBM)
GRANT = 20 << 20


def rows_needed(depth_out):
    deepest = depth_out + (ANGLES - 1) * HALF // ANGLES
    return -(-deepest // 8) * 8


def fields_of(shots, src_ref, rec_ref):
    return [(src_ref, s) for s in range(shots)] + [(rec_ref, s) for s in range(shots)]


def advance(step, x, c, beside, before, csq, shots, f, scalars, store):
    depth, ny = c.shape
    row = lax.broadcasted_iota(jnp.int32, (depth, ny), 0)
    lane = lax.broadcasted_iota(jnp.int32, (depth, ny), 1)
    beside = beside + jnp.where(row == 0, 0.0, pltpu.roll(c, 1, 0))
    beside = beside + jnp.where(row == depth - 1, 0.0, pltpu.roll(c, depth - 1, 0))
    beside = beside + jnp.where(lane == 0, 0.0, pltpu.roll(c, 1, 1))
    beside = beside + jnp.where(lane == ny - 1, 0.0, pltpu.roll(c, ny - 1, 1))
    store[...] = 2.0 * c - before + csq * (beside - 6.0 * c)
    lane1 = lax.broadcasted_iota(jnp.int32, (1, ny), 1)
    s = f % shots
    if f >= shots:
        line, value = receiver(scalars, s, step, x)
        add = jnp.where(lane1 == line, value, 0.0)
        store[0:1, :] = store[0:1, :] + add


def position(scalars, s, column):
    return scalars[1][s, column]


def receiver(scalars, s, step, x):
    return position(scalars, s, 3), scalars[3][s, STEPS - 1 - step, x]


def inject(step, scalars, planes, s, inside, row_of):
    at = position(scalars, s, 0) - scalars[0][0] * planes

    @pl.when(inside(at))
    def _():
        ref, index = row_of(at)
        z = (*index, pl.ds(position(scalars, s, 2), 1), slice(None))
        lane = lax.broadcasted_iota(jnp.int32, (1, ref.shape[-1]), 1)
        ref[z] = ref[z] + jnp.where(
            lane == position(scalars, s, 1), scalars[2][s, step], 0.0
        )


def inner_kernel(
    step, where_ref, pos_ref, wav_ref, tr_ref,
    src_ref, rec_ref, srcp_ref, recp_ref, csq_ref, lo_ref, hi_ref, srcn_ref, recn_ref,
):
    shots, planes, _, _ = src_ref.shape
    now = fields_of(shots, src_ref, rec_ref)
    prev = fields_of(shots, srcp_ref, recp_ref)
    nxt = fields_of(shots, srcn_ref, recn_ref)
    scalars = (where_ref, pos_ref, wav_ref, tr_ref)

    def plane(x, below, above):
        csq = csq_ref[x]
        for f in range(2 * shots):
            ref, s = now[f]
            out, _ = nxt[f]
            advance(
                step, x, ref[s, x], below(f) + above(f), prev[f][0][s, x], csq,
                shots, f, scalars, out.at[s, x],
            )

    def at(f, x):
        ref, s = now[f]
        return ref[s, x]

    plane(1, lambda f: lo_ref[f], lambda f: at(f, 2))
    plane(planes - 2, lambda f: at(f, planes - 3), lambda f: hi_ref[f])

    @pl.loop(2, planes - 2, unroll=2)
    def _(x):
        plane(x, lambda f: at(f, x - 1), lambda f: at(f, x + 1))

    for s in range(shots):
        inject(
            step, scalars, planes, s, lambda p: (p >= 1) & (p < planes - 1),
            lambda p, s=s: (srcn_ref, (s, p)),
        )


def first_kernel(
    step, where_ref, pos_ref, wav_ref, tr_ref,
    src_hbm, rec_hbm, srcp_hbm, recp_hbm, csq_hbm,
    src_ref, rec_ref, csq_ref, lo_ref, hi_ref, lop_ref, hip_ref, srcn_ref, recn_ref,
    srcp_ref, recp_ref, sem,
):
    moves = (
        (src_hbm, src_ref), (rec_hbm, rec_ref), (srcp_hbm, srcp_ref), (recp_hbm, recp_ref),
        (csq_hbm, csq_ref),
    )
    copies = [pltpu.make_async_copy(a, b, sem.at[n]) for n, (a, b) in enumerate(moves)]
    for copy in copies:
        copy.start()
    for copy in copies:
        copy.wait()
    shots, planes, _, _ = src_ref.shape
    for refs, low, high in (
        (fields_of(shots, src_ref, rec_ref), lo_ref, hi_ref),
        (fields_of(shots, srcp_ref, recp_ref), lop_ref, hip_ref),
    ):
        for f, (ref, s) in enumerate(refs):
            low[f] = ref[s, 0]
            high[f] = ref[s, planes - 1]
    inner_kernel(
        step, where_ref, pos_ref, wav_ref, tr_ref,
        src_ref, rec_ref, srcp_ref, recp_ref, csq_ref, lo_ref, hi_ref, srcn_ref, recn_ref,
    )


def edge_kernel(
    step, where_ref, pos_ref, wav_ref, tr_ref, src_ref, rec_ref, csq_ref,
    lo_ref, hi_ref, lop_ref, hip_ref, got_a_ref, got_b_ref, *outs
):
    shots, planes, _, _ = src_ref.shape
    now = fields_of(shots, src_ref, rec_ref)
    scalars = (where_ref, pos_ref, wav_ref, tr_ref)
    first = where_ref[1] == 0
    lon_ref, hin_ref = outs[:2]
    for f in range(2 * shots):
        ref, s = now[f]
        a = got_a_ref[f]
        b = got_b_ref[f]
        low = jnp.where(first, b, a)
        high = jnp.where(first, a, b)
        advance(
            step, 0, lo_ref[f], low + ref[s, 1], lop_ref[f], csq_ref[0],
            shots, f, scalars, lon_ref.at[f],
        )
        advance(
            step, planes - 1, hi_ref[f], high + ref[s, planes - 2], hip_ref[f], csq_ref[planes - 1],
            shots, f, scalars, hin_ref.at[f],
        )
    for s in range(shots):
        inject(step, scalars, planes, s, lambda p: p == 0, lambda p, s=s: (lon_ref, (s,)))
        inject(step, scalars, planes, s, lambda p: p == planes - 1, lambda p, s=s: (hin_ref, (s,)))
    if len(outs) > 2:
        edges(where_ref, lon_ref, hin_ref, outs[2], outs[3])


def edges(where_ref, lo_ref, hi_ref, a_ref, b_ref):
    first = where_ref[1] == 0
    for f in range(lo_ref.shape[0]):
        lo = lo_ref[f]
        hi = hi_ref[f]
        a_ref[f] = jnp.where(first, hi, lo)
        b_ref[f] = jnp.where(first, lo, hi)


def pack_kernel(
    where_ref, src_ref, rec_ref, lo_ref, hi_ref, keep_lo_ref, keep_hi_ref, near_ref, far_ref
):
    shots, planes, _, ny = src_ref.shape
    chunk, rows = keep_lo_ref.shape[1:3]
    width = ny // shots
    left = lax.broadcasted_iota(jnp.int32, (rows, ny), 1) < width
    first = where_ref[1] == 0

    def pack(a, b):
        lows = jnp.where(left, a, pltpu.roll(b, width, 1))
        highs = jnp.where(left, pltpu.roll(a, width, 1), b)
        return jnp.where(first, lows, highs), jnp.where(first, highs, lows)

    for field, ref in enumerate((src_ref, rec_ref)):
        f = field * shots

        def plane(x):
            if x == 0:
                return [lo_ref[f + s, :rows] for s in range(2)]
            if x == planes - 1:
                return [hi_ref[f + s, :rows] for s in range(2)]
            return [ref[s, x, :rows] for s in range(2)]

        for i in range(chunk):
            keep, low = pack(*plane(i))
            keep_lo_ref[field, i] = keep
            keep, high = pack(*plane(chunk + i))
            keep_hi_ref[field, i] = keep
            near_ref[field, i] = jnp.where(first, high, low)
            far_ref[field, i] = jnp.where(first, low, high)


def gather_window(where_ref, keep_lo, keep_hi, near, far, belows, aboves, win_ref):
    chunk = keep_lo.shape[1]
    odd = where_ref[1]
    even = 1 - odd
    own = HALF + odd * 2 * chunk
    over = HALF + 4 * chunk

    def place(piece, at):
        for i in range(chunk):
            for field in range(2):
                win_ref[field, at + i] = piece[field, i]

    place(keep_lo, own)
    place(keep_hi, own + chunk)
    place(near, HALF + chunk + even * chunk)
    place(far, HALF + even * 3 * chunk)
    place(belows[1], chunk)
    place(aboves[1], over + chunk)
    place(belows[0], odd * 2 * chunk)
    place(belows[2], even * 2 * chunk)
    place(aboves[0], over + odd * 2 * chunk)
    place(aboves[2], over + even * 2 * chunk)


def slants(win_ref, j_ref, d_ref, x, depth_out):
    tile = 8
    plan = [[] for _ in range(ANGLES)]
    slot = 0

    def load(field, p, r):
        return win_ref[field, p, tile * r : tile * (r + 1), :]

    def cross(u, v):
        return u[0] * v[1] + v[0] * u[1]

    for h in range(0, HALF + 1, 2):
        single = h + 1 > HALF
        top = h if single else h + 1
        tiles = -(-(depth_out + (ANGLES - 1) * top // ANGLES) // tile)
        moves = [angle * h // ANGLES for angle in range(ANGLES)]
        gaps = [0 if single else angle * (h + 1) // ANGLES - moves[angle] for angle in range(ANGLES)]
        slots = {gap: slot + k for k, gap in enumerate(sorted(set(gaps)))}
        slot += len(slots)
        for angle in range(ANGLES):
            plan[angle].append((slots[gaps[angle]], moves[angle]))
        base = HALF + x
        for r in reversed(range(tiles)):
            rows = slice(tile * r, tile * (r + 1))
            lower = slice(tile * r + 1, tile * (r + 1) + 1)
            if single:
                for k in range(2):
                    u = [load(field, base + k - h, r) for field in range(2)]
                    v = [load(field, base + k + h, r) for field in range(2)]
                    d_ref[k, slots[0], rows, :] = cross(u, v)
                continue
            us = [[load(field, base - h - 1 + k, r) for field in range(2)] for k in range(3)]
            vs = [[load(field, base + h + k, r) for field in range(2)] for k in range(3)]
            for k in range(2):
                if h == 0:
                    one = vs[k][0] * vs[k][1]
                else:
                    one = cross(us[1 + k], vs[k])
                two = cross(us[k], vs[1 + k])
                d_ref[k, slots[0], rows, :] = one + two
                if 1 in slots:
                    j_ref[k, h // 2, rows, :] = two
                    d_ref[k, slots[1], rows, :] = one + j_ref[k, h // 2, lower, :]

    def total(k, angle):
        value = None
        for at, moved in plan[angle]:
            piece = d_ref[k, at, moved : moved + depth_out, :]
            value = piece if value is None else value + piece
        return value

    return total


def image_kernel(parts, has_old, has_win, where_ref, *refs):
    refs = list(refs)
    j_ref, d_ref = refs[-2:]
    count = 1 if has_win else 10
    pieces = refs[:count]
    refs = refs[count:-2]
    olds = refs[: 2 * len(parts)] if has_old else None
    outs = refs[2 * len(parts) :] if has_old else refs
    if has_win:
        win_ref = pieces[0]
    else:
        win_ref = outs[-1]
        gather_window(where_ref, *pieces[:4], pieces[4:7], pieces[7:], win_ref)
    _, chunk, depth_out, ny = outs[0].shape
    width = ny // 2
    y = where_ref[1]
    core = where_ref[2]
    left = lax.broadcasted_iota(jnp.int32, (depth_out, ny), 1) < width
    group = ANGLES // 2

    def fold(v):
        return v + pltpu.roll(v, width, 1)

    for n, part in enumerate(parts):
        slab = y if part == "keep" else 1 - y
        mine_ref, theirs_ref = outs[2 * n], outs[2 * n + 1]

        @pl.loop(0, chunk)
        def _(i):
            total = slants(win_ref, j_ref, d_ref, slab * 2 * chunk + 2 * i, depth_out)

            def packed(angle):
                return jnp.where(left, fold(total(0, angle)), fold(total(1, angle)))

            for j in range(group):
                a = packed(j)
                b = packed(group + j)
                mine = jnp.where(core == 0, a, b)
                theirs = jnp.where(core == 0, b, a)
                if has_old:
                    mine = mine + olds[2 * n][j, i]
                    theirs = theirs + olds[2 * n + 1][j, i]
                mine_ref[j, i] = mine
                theirs_ref[j, i] = theirs


def final_kernel(scale, where_ref, keep_ref, other_ref, swap_ref, out_ref):
    angles, chunk, depth_out, ny = keep_ref.shape
    width = ny // 2
    left = lax.broadcasted_iota(jnp.int32, (depth_out, ny), 1) < width
    first = where_ref[1] == 0

    @pl.loop(0, chunk)
    def _(i):
        for a in range(angles):
            own = (keep_ref[a, i] + other_ref[a, i]) * scale
            got = swap_ref[a, i] * scale
            lows = jnp.where(first, own, got)
            highs = jnp.where(first, got, own)
            out_ref[a, 2 * i] = jnp.where(left, lows, pltpu.roll(highs, width, 1))
            out_ref[a, 2 * i + 1] = jnp.where(left, pltpu.roll(lows, width, 1), highs)


def call(kernel, out_shape, n_smem, args, scratch=(), flops=1_000_000, space=VMEM, grant=GRANT):
    return pl.pallas_call(
        kernel,
        out_shape=out_shape,
        in_specs=[SMEM] * n_smem + [space] * (len(args) - n_smem),
        out_specs=jax.tree.map(lambda _: VMEM, out_shape),
        scratch_shapes=list(scratch),
        cost_estimate=pl.CostEstimate(flops=flops, bytes_accessed=1_000_000, transcendentals=0),
        compiler_params=pltpu.CompilerParams(vmem_limit_bytes=grant),
    )(*args)


def local(src_now, src_prev, rec_now, rec_prev, courant_sq, wavelet, traces, positions):
    shots, planes, depth, ny = src_now.shape
    depth_out = depth // 2
    rows = min(depth, rows_needed(depth_out))
    chunk = planes // 2
    assert shots == 2 and HALF == 3 * chunk and planes == 2 * chunk and chunk % 2 == 0
    count = lax.axis_size("gx")
    assert count % 2 == 0
    here = lax.axis_index("gx")
    where = jnp.stack([here, here % 2, lax.axis_index("shot")]).astype(jnp.int32)
    even = here % 2 == 0
    f32 = jnp.float32
    shape = jax.ShapeDtypeStruct
    pair = [(i, i ^ 1) for i in range(count)]
    other_pair = [(i, (i - 1 ^ 1) + 1) for i in range(1, count - 1)]

    def send(value, pairs, axis="gx"):
        return lax.ppermute(value, axis, pairs)

    def hop(value, steps):
        return send(value, [(i, i + steps) for i in range(count) if 0 <= i + steps < count])

    edge = shape((2 * shots, depth, ny), f32)
    field = shape(src_now.shape, f32)
    half_piece = shape((2, chunk, rows, ny), f32)
    window = shape((2, 2 * planes + 2 * HALF + 1, rows, ny), f32)
    half_image = shape((ANGLES // 2, chunk, depth_out, ny), f32)
    scratch = [
        pltpu.VMEM((2, HALF // 2 + 1, rows + 8, ny), f32),
        pltpu.VMEM((2, HALF + 1, rows, ny), f32),
    ]
    scalars = (where, positions, wavelet, traces)

    lo = jnp.concatenate([src_now[:, 0], rec_now[:, 0]])
    hi = jnp.concatenate([src_now[:, -1], rec_now[:, -1]])
    a = jnp.where(even, hi, lo)
    b = jnp.where(even, lo, hi)
    every = STEPS // IMAGES
    src, rec = src_now, rec_now
    halos = (send(a, pair), send(b, other_pair))
    total = None
    for step in range(STEPS):
        if step == 0:
            kept = [field, field, shape(courant_sq.shape, f32)]
            src, rec, courant_sq, lo, hi, lo_prev, hi_prev, src_next, rec_next = call(
                functools.partial(first_kernel, step),
                kept + [edge] * 4 + [field] * 2, 4,
                scalars + tuple(
                    pltpu.with_memory_space_constraint(v, pltpu.HBM)
                    for v in (src, rec, src_prev, rec_prev, courant_sq)
                ),
                [pltpu.VMEM(src.shape, f32)] * 2 + [pltpu.SemaphoreType.DMA((5,))], space=HBM,
            )
        else:
            src_next, rec_next = call(
                functools.partial(inner_kernel, step), [field] * 2, 4,
                scalars + (src, rec, src_prev, rec_prev, courant_sq, lo, hi),
            )
        more = step + 1 < STEPS
        got = call(
            functools.partial(edge_kernel, step), [edge] * (4 if more else 2), 4,
            scalars + (src, rec, courant_sq, lo, hi, lo_prev, hi_prev) + halos,
        )
        src_prev, rec_prev, lo_prev, hi_prev = src, rec, lo, hi
        src, rec, lo, hi = src_next, rec_next, got[0], got[1]
        if more:
            halos = (send(got[2], pair), send(got[3], other_pair))
        if (step + 1) % every:
            continue
        keep_lo, keep_hi, near, far = call(
            pack_kernel, [half_piece] * 4, 1, (where, src, rec, lo, hi)
        )
        near = send(near, pair)
        far = send(far, pair)
        near_late, _ = lax.optimization_barrier((near, far))
        belows = (
            hop(keep_hi, 2),
            hop(jnp.where(even, near, keep_lo), 2),
            hop(jnp.where(even, far, near_late), 2),
        )
        aboves = (
            hop(keep_lo, -2),
            hop(jnp.where(even, keep_hi, near), -2),
            hop(jnp.where(even, near_late, far), -2),
        )
        pieces = (keep_lo, keep_hi, near, far) + belows + aboves
        if more:
            *total, _ = call(
                functools.partial(image_kernel, ("send", "keep"), total is not None, False),
                [half_image] * 4 + [window], 1, (where,) + pieces + tuple(total or ()), scratch,
                flops=60_000_000,
            )
    both = [(0, 1), (1, 0)]
    mine_send, theirs_send, win = call(
        functools.partial(image_kernel, ("send",), True, False),
        [half_image] * 2 + [window], 1, (where,) + pieces + tuple(total[:2]), scratch,
        flops=30_000_000,
    )
    got_send = send(theirs_send, both, "shot")
    swapped = send(mine_send + got_send, pair)
    mine_keep, theirs_keep = call(
        functools.partial(image_kernel, ("keep",), True, True),
        [half_image] * 2, 1, (where, win) + tuple(total[2:]), scratch,
        flops=30_000_000,
    )
    got_keep = send(theirs_keep, both, "shot")
    shots_all = shots * lax.axis_size("shot")
    scale = 1.0 / math.sqrt(LAGS * shots_all * IMAGES)
    return call(
        functools.partial(final_kernel, scale),
        shape((ANGLES // 2, planes, depth_out, ny), f32), 1,
        (where, mine_keep, got_keep, swapped),
    )


def solution(mesh):
    placed = (
        P(("groups", "shot"), "gx", None, None),
        P(("groups", "shot"), "gx", None, None),
        P(("groups", "shot"), "gx", None, None),
        P(("groups", "shot"), "gx", None, None),
        P(("groups", "gx"), None, None),
        P(("groups", "shot"), None),
        P(("groups", "shot"), None, "gx"),
        P(("groups", "shot"), None),
    )
    return jax.shard_map(
        local,
        mesh=mesh,
        in_specs=placed,
        out_specs=P(("groups", "shot"), "gx", None, None),
        check_vma=False,
    )
```
